512 devices in a mesh: gx: 64 (over y, z_lo, core), gy: 8 (over x, z_hi).
Axes of the slice: x: 4, y: 8, z: 8 (z_hi: 2, z_lo: 4; z = z_hi * 4 + z_lo), core: 2. Of those that a mesh axis runs over, the one named last changes fastest.
Arguments:
- fluid_velocity: float32 [3, 256, 128, 128], P(None, 'gx', 'gy'), may hold values from -6 to 6
- particle_velocity: float32 [64, 8, 4, 3, 128], P('gx', 'gy'), may hold values from -6 to 6
- particle_volume: float32 [64, 8, 4, 128], P('gx', 'gy'), may hold values from 0.02 to 0.3
- satellite_cells: int32 [64, 8, 4, 29, 128], P('gx', 'gy'), may hold values from 0 to 13823, as said below
- live_blocks: int32 [64, 8], P('gx', 'gy'), may hold values from 1 to 4
Outputs:
- void_fraction: float32 [256, 128, 128], P('gx', 'gy')
- drag: float32 [64, 8, 4, 3, 128], P('gx', 'gy')
The draws below stay inside these ranges and needn't reach their ends.
Inputs may be any that keep to these rules, and one draw needn't show every extreme that they name: `satellite_cells`: each entry names a cell of the owning slab's tile of 4 x 16 x 128 cells extended by one layer on each side along x and y, flattened as described in the reference program. `live_blocks`: blocks from this number on hold no live particles.
All inputs are finite; a program needn't handle non-finite values.
Results may differ from the reference program's by a relative error of at most 0.00029.
Values sent between devices are 32-bit elements; how exact they have to be, the bound alone decides.
No kernel may reach another device: no remote copies, remote signals or barrier semaphores. Data moves between devices by JAX's collectives and lax.ppermute only.
A program may use at most 64 MiB of HBM per device.

```python
import math
import jax
import jax.numpy as jnp

CX = 4
CY = 16
CZ = 128
BLOCKS = 4
SAT = 29
BLK = 128
NX = 256
NY = 128
NZ = 128
N_GX = 64
N_GY = 8


def draw_satellite_cells(key, part):
    keys = jax.random.split(jax.random.fold_in(key, 11), 6)
    block_shape = (N_GX, N_GY, BLOCKS, 1, 1)
    centre_shape = (3, N_GX, N_GY, BLOCKS, 1, BLK)
    full_shape = (3, N_GX, N_GY, BLOCKS, SAT, BLK)
    cluster_x = jax.random.randint(keys[0], block_shape, 0, CX + 2)
    cluster_y = jax.random.randint(keys[1], block_shape, 0, CY + 2)
    cluster_z = jax.random.randint(keys[2], block_shape, 0, CZ)
    centre_move = jax.random.randint(keys[3], centre_shape, -1, 2)
    offsets = jax.random.randint(keys[4], full_shape, -1, 2)
    moving = (jax.random.randint(keys[5], full_shape, 0, 4) == 0).astype(jnp.int32)
    steps = centre_move + offsets * moving
    layer_x = jnp.clip(cluster_x + steps[0], 0, CX + 1)
    layer_y = jnp.clip(cluster_y + steps[1], 0, CY + 1)
    layer_z = jnp.clip(cluster_z + steps[2], 0, CZ - 1)
    return ((layer_x * (CY + 2) + layer_y) * CZ + layer_z).astype(jnp.int32)


def plant(result, own_key, least, largest):
    index_at = [jax.random.randint(jax.random.fold_in(own_key, axis), (), 0, length) for axis, length in enumerate(result.shape)]
    main_axis = result.shape.index(max(result.shape))
    beside = index_at[:main_axis] + [(index_at[main_axis] + 1) % result.shape[main_axis]] + index_at[main_axis + 1:]
    return result.at[tuple(index_at)].set(least).at[tuple(beside)].set(largest)


def level_of(rng, extent, pieces, least, high):
    loudness = 1.0
    for axis_at, shards_of in pieces:
        heights = jax.random.uniform(jax.random.fold_in(jax.random.fold_in(rng, 6), axis_at), (shards_of,), jnp.float32, least / len(pieces), high / len(pieces))
        loudness = loudness * jnp.repeat(jnp.exp(heights), extent[axis_at] // shards_of).reshape((-1,) + (1,) * (len(extent) - 1 - axis_at))
    return loudness


def normal_values(stream_key, shape, spread, limit, cuts=(), kind=jnp.bfloat16):
    gain = level_of(stream_key, shape, cuts, -0.22, 0.18) if cuts else 1.0
    array = jax.random.normal(stream_key, shape, jnp.float32) * spread * gain
    return jnp.minimum(jnp.maximum(array, -limit), limit).astype(kind)


def setup_inputs(seed: int = 0) -> dict:
    splits = jax.random.split(jax.random.key(seed), 6)
    fluid_velocity = normal_values(splits[0], (3, NX, NY, NZ), 1.0, 6.0, ((1, 64), (2, 8)), jnp.float32)
    particle_velocity = normal_values(splits[1], (N_GX, N_GY, BLOCKS, 3, BLK), 1.0, 6.0, ((0, 64), (1, 8)), jnp.float32)
    particle_volume = jnp.clip(jnp.exp(math.log(0.3) - 2.7080503 * jax.random.uniform(splits[2], (N_GX, N_GY, BLOCKS, BLK), jnp.float32) ** level_of(splits[2], (N_GX, N_GY, BLOCKS, BLK), ((0, 64), (1, 8)), -0.2, 0.2)), 0.02, 0.3)
    satellite_cells = draw_satellite_cells(jax.random.fold_in(splits[5], 71), 0)
    live_blocks = plant(jax.random.randint(splits[4], (N_GX, N_GY), 1, BLOCKS + 1), jax.random.fold_in(splits[4], 1), 1, BLOCKS).astype(jnp.int32)
    return dict(fluid_velocity=fluid_velocity, particle_velocity=particle_velocity, particle_volume=particle_volume, satellite_cells=satellite_cells, live_blocks=live_blocks)


exponent = -2.65
drag_scale = 2.0
void_floor = 0.1


def reference(fluid_velocity, particle_velocity, particle_volume, satellite_cells, live_blocks):
    wide_y = CY + 2
    slab_x = jnp.arange(N_GX, dtype=jnp.int32)[:, None, None, None, None]
    slab_y = jnp.arange(N_GY, dtype=jnp.int32)[None, :, None, None, None]
    layer_x = satellite_cells // (wide_y * CZ)
    layer_y = (satellite_cells // CZ) % wide_y
    layer_z = satellite_cells % CZ
    global_x = (slab_x * CX + layer_x - 1) % NX
    global_y = (slab_y * CY + layer_y - 1) % NY
    flat_cell = ((global_x * NY + global_y) * NZ + layer_z).astype(jnp.int32)
    block_ids = jnp.arange(BLOCKS, dtype=jnp.int32)[None, None, :]
    alive = (block_ids < live_blocks[:, :, None]).astype(jnp.float32)
    volume_share = particle_volume * alive[..., None] / SAT
    weights = jnp.broadcast_to(volume_share[:, :, :, None, :], satellite_cells.shape)
    solid_volume = jnp.zeros((NX * NY * NZ,), jnp.float32).at[flat_cell.reshape(-1)].add(weights.reshape(-1))
    void_flat = jnp.maximum(1.0 - solid_volume, void_floor)
    resistance = void_flat ** exponent
    weight_at = resistance[flat_cell]
    weight_sum = jnp.sum(weight_at, axis=3)
    flow = fluid_velocity.reshape(3, -1)
    forces = []
    for component in range(3):
        pulling = jnp.sum(weight_at * flow[component][flat_cell], axis=3)
        moving = particle_velocity[:, :, :, component, :]
        forces.append(drag_scale * volume_share * (pulling - moving * weight_sum))
    drag = jnp.stack(forces, axis=3)
    return void_flat.reshape(NX, NY, NZ), drag
```

```python
import functools

import jax
import jax.numpy as jnp
from jax import lax
from jax.experimental import pallas as pl
from jax.experimental.pallas import tpu as pltpu
from jax.sharding import PartitionSpec as P

exponent = -2.65
drag_scale = 2.0
void_floor = 0.1

cells_x, cells_y, cells_z = 4, 16, 128
wide_y = cells_y + 2
inner_rows = cells_x * cells_y
x_low, x_high = inner_rows, inner_rows + cells_y
y_low, y_high = inner_rows + 2 * cells_y, inner_rows + 2 * cells_y + 8
tile_rows = y_high + 8
x_rows, y_rows = 88, 40


def split_cells(cells):
    lane = cells & (cells_z - 1)
    column = cells >> 7
    i = (column * 3641) >> 16
    j = column - i * wide_y
    inner = (i - 1) * cells_y + (j - 1)
    row = jnp.where(i == 0, x_low + j - 1, jnp.where(i == cells_x + 1, x_high + j - 1, inner))
    row = jnp.where(j == 0, y_low + i, jnp.where(j == cells_y + 1, y_high + i, row))
    return row, lane


def shares(live, volume, block, points):
    alive = jnp.where(block < live, 1.0, 0.0)
    return volume[block : block + 1] * alive / points


def halves(value):
    high = value.astype(jnp.bfloat16)
    low = (value - high.astype(jnp.float32)).astype(jnp.bfloat16)
    return high, low


def points_of(blocks, points):
    every = [(b, s) for b in range(blocks) for s in range(points)]
    return [every[at : at + 2] for at in range(0, len(every), 2)]


def deposit_kernel(live_ref, cells_ref, volume_ref, velocity_ref, tile_ref, up_ref, down_ref):
    blocks, points = cells_ref.shape[0], cells_ref.shape[1]
    live = live_ref[0, 0]
    volume = volume_ref[...]
    row_at = lax.broadcasted_iota(jnp.int32, (tile_rows, 128), 0).astype(jnp.float32).astype(jnp.bfloat16)
    lane_at = lax.broadcasted_iota(jnp.int32, (cells_z, 128), 0).astype(jnp.float32).astype(jnp.bfloat16)
    rows, lanes, high, low = [], [], [], []
    for b in range(blocks):
        row, lane = split_cells(cells_ref[b])
        rows.append(row.astype(jnp.float32).astype(jnp.bfloat16))
        lanes.append(lane.astype(jnp.float32).astype(jnp.bfloat16))
        h, l = halves(shares(live, volume, b, points))
        high.append(h)
        low.append(l)
    one = jnp.ones((), jnp.bfloat16)
    zero = jnp.zeros((), jnp.bfloat16)
    total = jnp.zeros((tile_rows, 2 * cells_z), jnp.float32)
    for pair in points_of(blocks, points):
        left, right = [], []
        for b, s in pair:
            left.append(jnp.where(row_at == rows[b][s : s + 1], one, zero))
            at_lane = lane_at == lanes[b][s : s + 1]
            right.append(
                jnp.concatenate([jnp.where(at_lane, high[b], zero), jnp.where(at_lane, low[b], zero)], axis=0)
            )
        total += lax.dot_general(
            jnp.concatenate(left, axis=1),
            jnp.concatenate(right, axis=1),
            (((1,), (1,)), ((), ())),
            preferred_element_type=jnp.float32,
        )
    tile_ref[...] = total[:, :cells_z] + total[:, cells_z:]

    def fill(out_ref, edge, beyond, layers, velocity_layer):
        first = (layers[0] - 1) * cells_y if 1 <= layers[0] <= cells_x else edge
        second = (layers[1] - 1) * cells_y if 1 <= layers[1] <= cells_x else edge
        out_ref[0:16] = tile_ref[first : first + 16]
        out_ref[16:32] = tile_ref[second : second + 16]
        out_ref[32:40] = jnp.zeros((8, 128), jnp.float32)
        out_ref[32:34] = tile_ref[y_low + layers[0] : y_low + layers[0] + 2]
        out_ref[34:36] = tile_ref[y_high + layers[0] : y_high + layers[0] + 2]
        for f in range(3):
            out_ref[40 + 16 * f : 56 + 16 * f] = velocity_ref[f, velocity_layer]

    fill(up_ref, x_high, None, (cells_x, cells_x + 1), cells_x - 1)
    fill(down_ref, x_low, None, (0, 1), 0)


def middle_kernel(tile_ref, velocity_ref, below_ref, above_ref, out_ref, up_ref, down_ref):
    out_ref[...] = tile_ref[...]
    out_ref[x_low : x_low + 16] += below_ref[0:16]
    out_ref[0:16] += below_ref[16:32]
    out_ref[y_low : y_low + 2] += below_ref[32:34]
    out_ref[y_high : y_high + 2] += below_ref[34:36]
    last = inner_rows - 16
    out_ref[last : last + 16] += above_ref[0:16]
    out_ref[x_high : x_high + 16] += above_ref[16:32]
    out_ref[y_low + 4 : y_low + 6] += above_ref[32:34]
    out_ref[y_high + 4 : y_high + 6] += above_ref[34:36]

    def fill(dest_ref, near, halo, order):
        dest_ref[...] = jnp.zeros((y_rows, 128), jnp.float32)
        at = 8 * order[0]
        dest_ref[at : at + 1] = out_ref[x_low + near : x_low + near + 1]
        for i in range(cells_x):
            dest_ref[at + 1 + i : at + 2 + i] = out_ref[16 * i + near : 16 * i + near + 1]
        dest_ref[at + 5 : at + 6] = out_ref[x_high + near : x_high + near + 1]
        at = 8 * order[1]
        dest_ref[at : at + 6] = out_ref[halo : halo + 6]
        for f in range(3):
            at = 16 + 8 * f
            dest_ref[at : at + 1] = below_ref[40 + 16 * f + near : 41 + 16 * f + near]
            for i in range(cells_x):
                dest_ref[at + 1 + i : at + 2 + i] = velocity_ref[f, i, near : near + 1]
            dest_ref[at + 5 : at + 6] = above_ref[40 + 16 * f + near : 41 + 16 * f + near]

    fill(up_ref, cells_y - 1, y_high, (0, 1))
    fill(down_ref, 0, y_low, (0, 1))


def drag_kernel(
    live_ref,
    cells_ref,
    volume_ref,
    particle_ref,
    velocity_ref,
    tile_ref,
    x_below_ref,
    x_above_ref,
    y_below_ref,
    y_above_ref,
    void_ref,
    drag_ref,
    solid_ref,
):
    blocks, points = cells_ref.shape[0], cells_ref.shape[1]
    live = live_ref[0, 0]
    volume = volume_ref[...]
    solid_ref[...] = tile_ref[...]

    def take_in(source_ref, near, halo):
        solid_ref[halo : halo + 6] += source_ref[0:6]
        solid_ref[x_low + near : x_low + near + 1] += source_ref[8:9]
        for i in range(cells_x):
            solid_ref[16 * i + near : 16 * i + near + 1] += source_ref[9 + i : 10 + i]
        solid_ref[x_high + near : x_high + near + 1] += source_ref[13:14]

    take_in(y_below_ref, 0, y_low)
    take_in(y_above_ref, cells_y - 1, y_high)
    void = jnp.maximum(1.0 - solid_ref[...], void_floor)
    for i in range(cells_x):
        void_ref[i] = void[16 * i : 16 * i + 16]
    resistance = jnp.exp(exponent * jnp.log(void))
    fields = [resistance]
    for f in range(3):
        flow = jnp.concatenate(
            [velocity_ref[f, i] for i in range(cells_x)]
            + [
                x_below_ref[40 + 16 * f : 56 + 16 * f],
                x_above_ref[40 + 16 * f : 56 + 16 * f],
                y_below_ref[16 + 8 * f : 24 + 8 * f],
                y_above_ref[16 + 8 * f : 24 + 8 * f],
            ],
            axis=0,
        )
        fields.append(resistance * flow)
    table = jnp.concatenate(fields, axis=0)
    table = jnp.concatenate(list(halves(table)), axis=1)

    row_at = lax.broadcasted_iota(jnp.int32, (tile_rows, 128), 0)
    lane_at = lax.broadcasted_iota(jnp.int32, (cells_z, 128), 0).astype(jnp.float32).astype(jnp.bfloat16)
    one = jnp.ones((), jnp.bfloat16)
    zero = jnp.zeros((), jnp.bfloat16)
    rows, lanes = [], []
    for b in range(blocks):
        row, lane = split_cells(cells_ref[b])
        rows.append(row)
        lanes.append(lane.astype(jnp.float32).astype(jnp.bfloat16))
    sums = [[jnp.zeros((8, 128), jnp.float32) for _ in range(4)] for _ in range(blocks)]
    for pair in points_of(blocks, points):
        right = [jnp.where(lane_at == lanes[b][s : s + 1], one, zero) for b, s in pair]
        right = jnp.concatenate(right, axis=1)
        found = jnp.dot(table, jnp.concatenate([right, right], axis=0), preferred_element_type=jnp.float32)
        for n, (b, s) in enumerate(pair):
            at_row = row_at == rows[b][s : s + 1]
            for f in range(4):
                part = found[f * tile_rows : (f + 1) * tile_rows, n * 128 : n * 128 + 128]
                part = jnp.where(at_row, part, 0.0)
                sums[b][f] = sums[b][f] + jnp.sum(part.reshape(tile_rows // 8, 8, 128), axis=0)
    for b in range(blocks):
        share = shares(live, volume, b, points)
        weight = jnp.sum(sums[b][0], axis=0, keepdims=True)
        for f in range(3):
            pulling = jnp.sum(sums[b][f + 1], axis=0, keepdims=True)
            drag_ref[b, f : f + 1] = drag_scale * share * (pulling - particle_ref[b, f : f + 1] * weight)


def on_chip(count):
    return [pl.BlockSpec(memory_space=pltpu.VMEM)] * count


def rows_of(count):
    return jax.ShapeDtypeStruct((count, 128), jnp.float32)


def both_ways(up, down, axis):
    count = lax.axis_size(axis)
    below = lax.ppermute(up, axis, [(i, (i + 1) % count) for i in range(count)])
    above = lax.ppermute(down, axis, [((i + 1) % count, i) for i in range(count)])
    return below, above


def body(fluid_velocity, particle_velocity, particle_volume, satellite_cells, live_blocks):
    cells = satellite_cells[0, 0]
    volume = particle_volume[0, 0]
    particles = particle_velocity[0, 0]
    blocks = cells.shape[0]
    scalar = pl.BlockSpec(memory_space=pltpu.SMEM)
    tile, x_up, x_down = pl.pallas_call(
        deposit_kernel,
        out_shape=(rows_of(tile_rows), rows_of(x_rows), rows_of(x_rows)),
        in_specs=[scalar] + on_chip(3),
        out_specs=tuple(on_chip(3)),
        name="deposit",
    )(live_blocks, cells, volume, fluid_velocity)
    x_below, x_above = both_ways(x_up, x_down, "gx")
    tile, y_up, y_down = pl.pallas_call(
        middle_kernel,
        out_shape=(rows_of(tile_rows), rows_of(y_rows), rows_of(y_rows)),
        in_specs=on_chip(4),
        out_specs=tuple(on_chip(3)),
        name="middle",
    )(tile, fluid_velocity, x_below, x_above)
    y_below, y_above = both_ways(y_up, y_down, "gy")
    void, drag = pl.pallas_call(
        drag_kernel,
        out_shape=(
            jax.ShapeDtypeStruct((cells_x, cells_y, cells_z), jnp.float32),
            jax.ShapeDtypeStruct((blocks, 3, 128), jnp.float32),
        ),
        in_specs=[scalar] + on_chip(9),
        out_specs=tuple(on_chip(2)),
        scratch_shapes=[pltpu.VMEM((tile_rows, 128), jnp.float32)],
        name="drag",
    )(live_blocks, cells, volume, particles, fluid_velocity, tile, x_below, x_above, y_below, y_above)
    return void, drag[None, None]


def solution(mesh):
    placed = (
        P(None, "gx", "gy", None),
        P("gx", "gy", None, None, None),
        P("gx", "gy", None, None),
        P("gx", "gy", None, None, None),
        P("gx", "gy"),
    )
    return jax.shard_map(
        body,
        mesh=mesh,
        in_specs=placed,
        out_specs=(P("gx", "gy", None), P("gx", "gy", None, None, None)),
        check_vma=False,
    )
```

```python
import jax
import jax.numpy as jnp
from jax import lax
from jax.experimental import pallas as pl
from jax.experimental.pallas import tpu as pltpu
from jax.sharding import PartitionSpec as P

exponent = -2.65
drag_scale = 2.0
void_floor = 0.1

cells_x, cells_y, cells_z = 4, 16, 128
wide_x, wide_y = cells_x + 2, cells_y + 2
own_y = wide_y - 4
late_rows = 4 * wide_x
early_rows = wide_x * own_y
early_padded = 88
tile_rows = 112
x_rows, x_flow, y_rows, y_flow = 88, 40, 40, 16


def split_cells(cells):
    lane = cells & (cells_z - 1)
    column = cells >> 7
    i = (column * 3641) >> 16
    j = column - i * wide_y
    late = jnp.where(j < 2, j, j - own_y) * wide_x + i
    early = late_rows + i * own_y + (j - 2)
    row = jnp.where((j < 2) | (j >= wide_y - 2), late, early)
    return row, lane


def points_in(cells_ref, block):
    return jnp.concatenate([cells_ref[s, block : block + 1] for s in range(cells_ref.shape[0])], axis=0)


def halves(value):
    high = value.astype(jnp.bfloat16)
    low = (value - high.astype(jnp.float32)).astype(jnp.bfloat16)
    return high, low


def counted(rows):
    return lax.broadcasted_iota(jnp.int32, (rows, 128), 0)


def narrow(value):
    return value.astype(jnp.float32).astype(jnp.bfloat16)


def pairs_of(block, points):
    every = [(block, s) for s in range(points)]
    return [every[at : at + 2] for at in range(0, points, 2)]


def deposit_kernel(
    live_ref, cells_ref, volume_ref, velocity_ref, tile_ref, up_ref, down_ref, share_ref, cells_in, volume_in, live_in, sems
):
    points, blocks = cells_ref.shape[0], cells_ref.shape[1]
    copies = [
        pltpu.make_async_copy(cells_ref, cells_in, sems.at[0]),
        pltpu.make_async_copy(volume_ref, volume_in, sems.at[1]),
        pltpu.make_async_copy(live_ref, live_in, sems.at[2]),
    ]
    for f in range(3):
        at = pl.ds(x_flow + cells_y * f, cells_y)
        copies.append(pltpu.make_async_copy(velocity_ref.at[f, cells_x - 1], up_ref.at[at], sems.at[3 + f]))
        copies.append(pltpu.make_async_copy(velocity_ref.at[f, 0], down_ref.at[at], sems.at[6 + f]))
    for copy in copies:
        copy.start()
    row_at = narrow(counted(tile_rows))
    lane_at = narrow(counted(cells_z))
    one = jnp.ones((), jnp.bfloat16)
    zero = jnp.zeros((), jnp.bfloat16)
    copies[1].wait()
    share = volume_in[...] / points
    high, low = halves(share)
    copies[0].wait()
    totals = []
    for b in range(blocks):
        row, lane = split_cells(points_in(cells_in, b))
        row, lane = narrow(row), narrow(lane)
        total = jnp.zeros((2 * tile_rows, cells_z), jnp.float32)
        for pair in pairs_of(b, points):
            left, right = [], []
            for _, s in pair:
                at_row = row_at == row[s : s + 1]
                left.append(
                    jnp.concatenate(
                        [jnp.where(at_row, high[b : b + 1], zero), jnp.where(at_row, low[b : b + 1], zero)], axis=0
                    )
                )
                right.append(jnp.where(lane_at == lane[s : s + 1], one, zero))
            total += lax.dot_general(
                jnp.concatenate(left, axis=1),
                jnp.concatenate(right, axis=1),
                (((1,), (1,)), ((), ())),
                preferred_element_type=jnp.float32,
            )
        totals.append(total)
    copies[2].wait()
    live = live_in[0, 0]
    tile = jnp.zeros((tile_rows, cells_z), jnp.float32)
    for b in range(blocks):
        alive = jnp.where(b < live, 1.0, 0.0)
        tile += alive * (totals[b][:tile_rows] + totals[b][tile_rows:])
        share_ref[b : b + 1] = alive * share[b : b + 1]
    tile_ref[...] = tile
    up_ref[0:28] = tile_ref[80:108]
    down_ref[0:28] = tile_ref[24:52]
    for g in range(4):
        up_ref[28 + 2 * g : 30 + 2 * g] = tile_ref[6 * g + 4 : 6 * g + 6]
        down_ref[28 + 2 * g : 30 + 2 * g] = tile_ref[6 * g : 6 * g + 2]
    up_ref[36:40] = jnp.zeros((4, 128), jnp.float32)
    down_ref[36:40] = jnp.zeros((4, 128), jnp.float32)
    for copy in copies[3:]:
        copy.wait()


def middle_kernel(tile_ref, velocity_ref, below_ref, above_ref, out_ref, up_ref, down_ref):
    out_ref[...] = tile_ref[...]
    out_ref[24:52] += below_ref[0:28]
    out_ref[80:108] += above_ref[0:28]
    for g in range(4):
        out_ref[6 * g : 6 * g + 2] += below_ref[28 + 2 * g : 30 + 2 * g]
        out_ref[6 * g + 4 : 6 * g + 6] += above_ref[28 + 2 * g : 30 + 2 * g]

    def fill(dest_ref, first, near):
        dest_ref[...] = jnp.zeros((y_rows, 128), jnp.float32)
        dest_ref[0:12] = out_ref[first : first + 12]
        for f in range(3):
            at, halo = y_flow + 8 * f, x_flow + cells_y * f + near
            dest_ref[at : at + 1] = below_ref[halo : halo + 1]
            for i in range(cells_x):
                dest_ref[at + 1 + i : at + 2 + i] = velocity_ref[f, i, near : near + 1]
            dest_ref[at + 5 : at + 6] = above_ref[halo : halo + 1]

    fill(up_ref, 12, cells_y - 1)
    fill(down_ref, 0, 0)


def looked_up(cells_ref, fields, first):
    points, blocks = cells_ref.shape[0], cells_ref.shape[1]
    rows = fields[0].shape[0]
    table = jnp.concatenate(list(halves(jnp.concatenate(fields, axis=0))), axis=1)
    row_at = counted(rows) + first
    lane_at = narrow(counted(cells_z))
    one = jnp.ones((), jnp.bfloat16)
    zero = jnp.zeros((), jnp.bfloat16)
    sums = []
    for b in range(blocks):
        row, lane = split_cells(points_in(cells_ref, b))
        lane = narrow(lane)
        part_sums = [jnp.zeros((8, 128), jnp.float32) for _ in fields]
        for pair in pairs_of(b, points):
            right = [jnp.where(lane_at == lane[s : s + 1], one, zero) for _, s in pair]
            right = jnp.concatenate(right, axis=1)
            found = jnp.dot(table, jnp.concatenate([right, right], axis=0), preferred_element_type=jnp.float32)
            for n, (_, s) in enumerate(pair):
                at_row = row_at == row[s : s + 1]
                for f in range(len(fields)):
                    part = jnp.where(at_row, found[f * rows : (f + 1) * rows, n * 128 : n * 128 + 128], 0.0)
                    part_sums[f] = part_sums[f] + jnp.sum(part.reshape(rows // 8, 8, 128), axis=0)
        sums.append([jnp.sum(part, axis=0, keepdims=True) for part in part_sums])
    return sums


def void_of(solid):
    return jnp.maximum(1.0 - solid, void_floor)


def resistance_of(void):
    return jnp.exp(exponent * jnp.log(void))


def early_kernel(cells_ref, velocity_ref, tile_ref, below_ref, above_ref, sums_ref):
    resistance = resistance_of(void_of(tile_ref[late_rows : late_rows + early_rows]))
    fields = [resistance]
    for f in range(3):
        halo = x_flow + cells_y * f + 1
        flow = [below_ref[halo : halo + own_y]]
        flow += [velocity_ref[f, i, 1 : 1 + own_y] for i in range(cells_x)]
        flow += [above_ref[halo : halo + own_y]]
        fields.append(resistance * jnp.concatenate(flow, axis=0))
    blank = jnp.zeros((early_padded - early_rows, 128), jnp.float32)
    fields = [jnp.concatenate([field, blank], axis=0) for field in fields]
    for b, sums in enumerate(looked_up(cells_ref, fields, late_rows)):
        for f in range(4):
            sums_ref[f, b : b + 1] = sums[f]


def drag_kernel(
    cells_ref, share_ref, particle_ref, tile_ref, up_ref, down_ref, below_ref, above_ref, sums_ref, void_ref, drag_ref
):
    late = jnp.concatenate(
        [tile_ref[0:12] + below_ref[0:12], tile_ref[12:24] + above_ref[0:12]], axis=0
    )
    late_void = void_of(late)
    early_void = void_of(tile_ref[late_rows : late_rows + early_rows])
    for i in range(1, cells_x + 1):
        void_ref[i - 1, 0:1] = late_void[wide_x + i : wide_x + i + 1]
        void_ref[i - 1, 1 : 1 + own_y] = early_void[i * own_y : (i + 1) * own_y]
        void_ref[i - 1, 1 + own_y : 2 + own_y] = late_void[2 * wide_x + i : 2 * wide_x + i + 1]
    resistance = resistance_of(late_void)
    fields = [resistance]
    for f in range(3):
        at = slice(y_flow + 8 * f, y_flow + 8 * f + wide_x)
        flow = jnp.concatenate([below_ref[at], down_ref[at], up_ref[at], above_ref[at]], axis=0)
        fields.append(resistance * flow)
    for b, sums in enumerate(looked_up(cells_ref, fields, 0)):
        total = [sums[f] + sums_ref[f, b : b + 1] for f in range(4)]
        for f in range(3):
            force = total[f + 1] - particle_ref[f, b : b + 1] * total[0]
            drag_ref[f, b : b + 1] = drag_scale * share_ref[b : b + 1] * force


def on_chip(count):
    return [pl.BlockSpec(memory_space=pltpu.VMEM)] * count


def array_of(*shape):
    return jax.ShapeDtypeStruct(shape, jnp.float32)


def both_ways(up, down, axis):
    count = lax.axis_size(axis)
    below = lax.ppermute(up, axis, [(i, (i + 1) % count) for i in range(count)])
    above = lax.ppermute(down, axis, [((i + 1) % count, i) for i in range(count)])
    return below, above


def small():
    return pltpu.CompilerParams(vmem_limit_bytes=16 * 1024 * 1024)


def body(fluid_velocity, particle_velocity, particle_volume, satellite_cells, live_blocks):
    cells = jnp.transpose(satellite_cells[0, 0], (1, 0, 2))
    volume = particle_volume[0, 0]
    particles = jnp.transpose(particle_velocity[0, 0], (1, 0, 2))
    blocks = volume.shape[0]
    tile, x_up, x_down, share = pl.pallas_call(
        deposit_kernel,
        out_shape=(array_of(tile_rows, 128), array_of(x_rows, 128), array_of(x_rows, 128), array_of(blocks, 128)),
        in_specs=[pl.BlockSpec(memory_space=pltpu.HBM)] * 4,
        out_specs=tuple(on_chip(4)),
        scratch_shapes=[
            pltpu.VMEM(cells.shape, jnp.int32),
            pltpu.VMEM(volume.shape, jnp.float32),
            pltpu.SMEM(live_blocks.shape, jnp.int32),
            pltpu.SemaphoreType.DMA((9,)),
        ],
        compiler_params=small(),
        name="deposit",
    )(live_blocks, *(pltpu.with_memory_space_constraint(value, pltpu.HBM) for value in (cells, volume, fluid_velocity)))
    x_below, x_above = both_ways(x_up, x_down, "gx")
    tile, y_up, y_down = pl.pallas_call(
        middle_kernel,
        out_shape=(array_of(tile_rows, 128), array_of(y_rows, 128), array_of(y_rows, 128)),
        in_specs=on_chip(4),
        out_specs=tuple(on_chip(3)),
        compiler_params=small(),
        name="middle",
    )(tile, fluid_velocity, x_below, x_above)
    y_below, y_above = both_ways(y_up, y_down, "gy")
    sums = pl.pallas_call(
        early_kernel,
        out_shape=array_of(4, blocks, 128),
        in_specs=on_chip(5),
        out_specs=on_chip(1)[0],
        compiler_params=small(),
        cost_estimate=pl.CostEstimate(flops=3_000_000_000, bytes_accessed=300_000, transcendentals=20_000),
        name="early",
    )(cells, fluid_velocity, tile, x_below, x_above)
    void, drag = pl.pallas_call(
        drag_kernel,
        out_shape=(array_of(cells_x, cells_y, cells_z), array_of(3, blocks, 128)),
        in_specs=on_chip(9),
        out_specs=tuple(on_chip(2)),
        compiler_params=small(),
        name="drag",
    )(cells, share, particles, tile, y_up, y_down, y_below, y_above, sums)
    return void, jnp.transpose(drag, (1, 0, 2))[None, None]


def solution(mesh):
    placed = (
        P(None, "gx", "gy", None),
        P("gx", "gy", None, None, None),
        P("gx", "gy", None, None),
        P("gx", "gy", None, None, None),
        P("gx", "gy"),
    )
    return jax.shard_map(
        body,
        mesh=mesh,
        in_specs=placed,
        out_specs=(P("gx", "gy", None), P("gx", "gy", None, None, None)),
        check_vma=False,
    )
```

```python
import functools

import jax
import jax.numpy as jnp
from jax import lax
from jax.experimental import pallas as pl
from jax.experimental.pallas import tpu as pltpu
from jax.sharding import PartitionSpec as P


exponent = -2.65
drag_scale = 2.0
void_floor = 0.1

cells_x, cells_y, cells_z = 4, 16, 128
wide_x, wide_y = cells_x + 2, cells_y + 2
own_y = wide_y - 4
late_rows = 4 * wide_x
early_rows = wide_x * own_y
early_padded = 88
tile_rows = 112
x_rows, x_flow, y_rows, y_flow = 88, 40, 40, 16


def split_cells(cells):
    lane = cells & (cells_z - 1)
    column = cells >> 7
    i = (column * 3641) >> 16
    j = column - i * wide_y
    late = jnp.where(j < 2, j, j - own_y) * wide_x + i
    early = late_rows + i * own_y + (j - 2)
    row = jnp.where((j < 2) | (j >= wide_y - 2), late, early)
    return row, lane


def points_in(cells_ref, block):
    return jnp.concatenate([cells_ref[s, block : block + 1] for s in range(cells_ref.shape[0])], axis=0)


def halves(value):
    high = value.astype(jnp.bfloat16)
    low = (value - high.astype(jnp.float32)).astype(jnp.bfloat16)
    return high, low


def counted(rows):
    return lax.broadcasted_iota(jnp.int32, (rows, 128), 0)


def narrow(value):
    return value.astype(jnp.float32).astype(jnp.bfloat16)


def pairs_of(block, points):
    every = [(block, s) for s in range(points)]
    return [every[at : at + 2] for at in range(0, points, 2)]


def deposit_kernel(
    live_ref, cells_ref, volume_ref, velocity_ref, tile_ref, up_ref, down_ref, share_ref, cells_in, volume_in, live_in, sems
):
    points, blocks = cells_ref.shape[0], cells_ref.shape[1]
    copies = [
        pltpu.make_async_copy(cells_ref, cells_in, sems.at[0]),
        pltpu.make_async_copy(volume_ref, volume_in, sems.at[1]),
        pltpu.make_async_copy(live_ref, live_in, sems.at[2]),
    ]
    for f in range(3):
        at = pl.ds(x_flow + cells_y * f, cells_y)
        copies.append(pltpu.make_async_copy(velocity_ref.at[f, cells_x - 1], up_ref.at[at], sems.at[3 + f]))
        copies.append(pltpu.make_async_copy(velocity_ref.at[f, 0], down_ref.at[at], sems.at[6 + f]))
    for copy in copies:
        copy.start()
    row_at = narrow(counted(tile_rows))
    lane_at = narrow(counted(cells_z))
    one = jnp.ones((), jnp.bfloat16)
    zero = jnp.zeros((), jnp.bfloat16)
    copies[1].wait()
    share = volume_in[...] / points
    high, low = halves(share)
    copies[0].wait()
    totals = []
    for b in range(blocks):
        row, lane = split_cells(points_in(cells_in, b))
        row, lane = narrow(row), narrow(lane)
        total = jnp.zeros((2 * tile_rows, cells_z), jnp.float32)
        for pair in pairs_of(b, points):
            left, right = [], []
            for _, s in pair:
                at_row = row_at == row[s : s + 1]
                left.append(
                    jnp.concatenate(
                        [jnp.where(at_row, high[b : b + 1], zero), jnp.where(at_row, low[b : b + 1], zero)], axis=0
                    )
                )
                right.append(jnp.where(lane_at == lane[s : s + 1], one, zero))
            total += lax.dot_general(
                jnp.concatenate(left, axis=1),
                jnp.concatenate(right, axis=1),
                (((1,), (1,)), ((), ())),
                preferred_element_type=jnp.float32,
            )
        totals.append(total)
    copies[2].wait()
    live = live_in[0, 0]
    tile = jnp.zeros((tile_rows, cells_z), jnp.float32)
    for b in range(blocks):
        alive = jnp.where(b < live, 1.0, 0.0)
        tile += alive * (totals[b][:tile_rows] + totals[b][tile_rows:])
        share_ref[b : b + 1] = alive * share[b : b + 1]
    tile_ref[...] = tile
    up_ref[0:28] = tile_ref[80:108]
    down_ref[0:28] = tile_ref[24:52]
    for g in range(4):
        up_ref[28 + 2 * g : 30 + 2 * g] = tile_ref[6 * g + 4 : 6 * g + 6]
        down_ref[28 + 2 * g : 30 + 2 * g] = tile_ref[6 * g : 6 * g + 2]
    up_ref[36:40] = jnp.zeros((4, 128), jnp.float32)
    down_ref[36:40] = jnp.zeros((4, 128), jnp.float32)
    for copy in copies[3:]:
        copy.wait()


def middle_kernel(tile_ref, velocity_ref, below_ref, above_ref, out_ref, up_ref, down_ref):
    out_ref[...] = tile_ref[...]
    out_ref[24:52] += below_ref[0:28]
    out_ref[80:108] += above_ref[0:28]
    for g in range(4):
        out_ref[6 * g : 6 * g + 2] += below_ref[28 + 2 * g : 30 + 2 * g]
        out_ref[6 * g + 4 : 6 * g + 6] += above_ref[28 + 2 * g : 30 + 2 * g]

    def fill(dest_ref, first, near):
        dest_ref[...] = jnp.zeros((y_rows, 128), jnp.float32)
        dest_ref[0:12] = out_ref[first : first + 12]
        for f in range(3):
            at, halo = y_flow + 8 * f, x_flow + cells_y * f + near
            dest_ref[at : at + 1] = below_ref[halo : halo + 1]
            for i in range(cells_x):
                dest_ref[at + 1 + i : at + 2 + i] = velocity_ref[f, i, near : near + 1]
            dest_ref[at + 5 : at + 6] = above_ref[halo : halo + 1]

    fill(up_ref, 12, cells_y - 1)
    fill(down_ref, 0, 0)


def looked_up(cells_ref, fields, first):
    points, blocks = cells_ref.shape[0], cells_ref.shape[1]
    rows = fields[0].shape[0]
    table = jnp.concatenate(list(halves(jnp.concatenate(fields, axis=0))), axis=1)
    row_at = counted(rows) + first
    lane_at = narrow(counted(cells_z))
    one = jnp.ones((), jnp.bfloat16)
    zero = jnp.zeros((), jnp.bfloat16)
    sums = []
    for b in range(blocks):
        row, lane = split_cells(points_in(cells_ref, b))
        lane = narrow(lane)
        part_sums = [jnp.zeros((8, 128), jnp.float32) for _ in fields]
        for pair in pairs_of(b, points):
            right = [jnp.where(lane_at == lane[s : s + 1], one, zero) for _, s in pair]
            right = jnp.concatenate(right, axis=1)
            found = jnp.dot(table, jnp.concatenate([right, right], axis=0), preferred_element_type=jnp.float32)
            for n, (_, s) in enumerate(pair):
                at_row = row_at == row[s : s + 1]
                for f in range(len(fields)):
                    part = jnp.where(at_row, found[f * rows : (f + 1) * rows, n * 128 : n * 128 + 128], 0.0)
                    part_sums[f] = part_sums[f] + jnp.sum(part.reshape(rows // 8, 8, 128), axis=0)
        sums.append([jnp.sum(part, axis=0, keepdims=True) for part in part_sums])
    return sums


def void_of(solid):
    return jnp.maximum(1.0 - solid, void_floor)


def resistance_of(void):
    return jnp.exp(exponent * jnp.log(void))


def on_side(side):
    return lax.rem(lax.axis_index("gy"), 2) == side


def early_kernel(side, cells_ref, velocity_ref, tile_ref, below_ref, above_ref, sums_ref):
    @pl.when(on_side(side))
    def _():
        resistance = resistance_of(void_of(tile_ref[late_rows : late_rows + early_rows]))
        fields = [resistance]
        for f in range(3):
            halo = x_flow + cells_y * f + 1
            flow = [below_ref[halo : halo + own_y]]
            flow += [velocity_ref[f, i, 1 : 1 + own_y] for i in range(cells_x)]
            flow += [above_ref[halo : halo + own_y]]
            fields.append(resistance * jnp.concatenate(flow, axis=0))
        blank = jnp.zeros((early_padded - early_rows, 128), jnp.float32)
        fields = [jnp.concatenate([field, blank], axis=0) for field in fields]
        for b, sums in enumerate(looked_up(cells_ref, fields, late_rows)):
            for f in range(4):
                sums_ref[f, b : b + 1] = sums[f]


def drag_kernel(side, *refs):
    cells_ref, share_ref, particle_ref, tile_ref, up_ref, down_ref, below_ref, above_ref, sums_ref = refs[:9]
    void_out, drag_out, void_ref, drag_ref, particle_in, sems = refs[-6:]

    @pl.when(on_side(side))
    def _():
        fetch = pltpu.make_async_copy(particle_ref, particle_in, sems.at[2])
        fetch.start()
        late = jnp.concatenate([tile_ref[0:12] + below_ref[0:12], tile_ref[12:24] + above_ref[0:12]], axis=0)
        late_void = void_of(late)
        early_void = void_of(tile_ref[late_rows : late_rows + early_rows])
        for i in range(1, cells_x + 1):
            void_ref[i - 1, 0:1] = late_void[wide_x + i : wide_x + i + 1]
            void_ref[i - 1, 1 : 1 + own_y] = early_void[i * own_y : (i + 1) * own_y]
            void_ref[i - 1, 1 + own_y : 2 + own_y] = late_void[2 * wide_x + i : 2 * wide_x + i + 1]
        resistance = resistance_of(late_void)
        fields = [resistance]
        for f in range(3):
            at = slice(y_flow + 8 * f, y_flow + 8 * f + wide_x)
            flow = jnp.concatenate([below_ref[at], down_ref[at], up_ref[at], above_ref[at]], axis=0)
            fields.append(resistance * flow)
        found = looked_up(cells_ref, fields, 0)
        fetch.wait()
        for b, sums in enumerate(found):
            total = [sums[f] + sums_ref[f, b : b + 1] for f in range(4)]
            for f in range(3):
                force = total[f + 1] - particle_in[f, b : b + 1] * total[0]
                drag_ref[f, b : b + 1] = drag_scale * share_ref[b : b + 1] * force
        copies = [
            pltpu.make_async_copy(void_ref, void_out, sems.at[0]),
            pltpu.make_async_copy(drag_ref, drag_out, sems.at[1]),
        ]
        for copy in copies:
            copy.start()
        for copy in copies:
            copy.wait()


def on_chip(count):
    return [pl.BlockSpec(memory_space=pltpu.VMEM)] * count


def array_of(*shape):
    return jax.ShapeDtypeStruct(shape, jnp.float32)


def both_ways(up, down, axis):
    count = lax.axis_size(axis)
    below = lax.ppermute(up, axis, [(i, (i + 1) % count) for i in range(count)])
    above = lax.ppermute(down, axis, [((i + 1) % count, i) for i in range(count)])
    return below, above


def one_way(value, axis, side, step):
    count = lax.axis_size(axis)
    return lax.ppermute(value, axis, [(i, (i + step) % count) for i in range(count) if i % 2 == side])


def early(side, values):
    return pl.pallas_call(
        functools.partial(early_kernel, side),
        out_shape=array_of(4, values[0].shape[1], 128),
        in_specs=on_chip(5),
        out_specs=on_chip(1)[0],
        compiler_params=small(),
        cost_estimate=pl.CostEstimate(flops=3_000_000_000, bytes_accessed=300_000, transcendentals=20_000),
    )(*values)


def drag_of(side, values, result):
    blocks = values[1].shape[0]
    in_hbm = pl.BlockSpec(memory_space=pltpu.HBM)
    return pl.pallas_call(
        functools.partial(drag_kernel, side),
        out_shape=(array_of(cells_x, cells_y, cells_z), array_of(3, blocks, 128)),
        in_specs=on_chip(2) + [in_hbm] + on_chip(6) + [in_hbm] * len(result),
        out_specs=(in_hbm,) * 2,
        scratch_shapes=[
            pltpu.VMEM((cells_x, cells_y, cells_z), jnp.float32),
            pltpu.VMEM((3, blocks, 128), jnp.float32),
            pltpu.VMEM((3, blocks, 128), jnp.float32),
            pltpu.SemaphoreType.DMA((3,)),
        ],
        input_output_aliases={9: 0, 10: 1} if result else {},
        compiler_params=small(),
    )(*values, *result)


def small():
    return pltpu.CompilerParams(vmem_limit_bytes=16 * 1024 * 1024)


def body(fluid_velocity, particle_velocity, particle_volume, satellite_cells, live_blocks):
    cells = jnp.transpose(satellite_cells[0, 0], (1, 0, 2))
    volume = particle_volume[0, 0]
    particles = jnp.transpose(particle_velocity[0, 0], (1, 0, 2))
    particles = pltpu.with_memory_space_constraint(particles, pltpu.HBM)
    blocks = volume.shape[0]
    tile, x_up, x_down, share = pl.pallas_call(
        deposit_kernel,
        out_shape=(array_of(tile_rows, 128), array_of(x_rows, 128), array_of(x_rows, 128), array_of(blocks, 128)),
        in_specs=[pl.BlockSpec(memory_space=pltpu.HBM)] * 4,
        out_specs=tuple(on_chip(4)),
        scratch_shapes=[
            pltpu.VMEM(cells.shape, jnp.int32),
            pltpu.VMEM(volume.shape, jnp.float32),
            pltpu.SMEM(live_blocks.shape, jnp.int32),
            pltpu.SemaphoreType.DMA((9,)),
        ],
        compiler_params=small(),
        name="deposit",
    )(live_blocks, *(pltpu.with_memory_space_constraint(value, pltpu.HBM) for value in (cells, volume, fluid_velocity)))
    x_below, x_above = both_ways(x_up, x_down, "gx")
    tile, y_up, y_down = pl.pallas_call(
        middle_kernel,
        out_shape=(array_of(tile_rows, 128), array_of(y_rows, 128), array_of(y_rows, 128)),
        in_specs=on_chip(4),
        out_specs=tuple(on_chip(3)),
        compiler_params=small(),
        name="middle",
    )(tile, fluid_velocity, x_below, x_above)
    below_even = one_way(y_up, "gy", 1, 1)
    above_even = one_way(y_down, "gy", 1, -1)
    early_in = (cells, fluid_velocity, tile, x_below, x_above)
    sums_even = early(0, early_in)
    below_odd = one_way(y_up, "gy", 0, 1)
    above_odd = one_way(y_down, "gy", 0, -1)
    sums_odd = early(1, early_in)
    rest = (cells, share, particles, tile, y_up, y_down)
    result = drag_of(0, rest + (below_even, above_even, sums_even), ())
    void, drag = drag_of(1, rest + (below_odd, above_odd, sums_odd), result)
    return void, jnp.transpose(drag, (1, 0, 2))[None, None]


def solution(mesh):
    placed = (
        P(None, "gx", "gy", None),
        P("gx", "gy", None, None, None),
        P("gx", "gy", None, None),
        P("gx", "gy", None, None, None),
        P("gx", "gy"),
    )
    return jax.shard_map(
        body,
        mesh=mesh,
        in_specs=placed,
        out_specs=(P("gx", "gy", None), P("gx", "gy", None, None, None)),
        check_vma=False,
    )
```

```python
import functools

import jax
import jax.numpy as jnp
from jax import lax
from jax.experimental import pallas as pl
from jax.experimental.pallas import tpu as pltpu
from jax.sharding import PartitionSpec as P


exponent = -2.65
drag_scale = 2.0
void_floor = 0.1

cells_x, cells_y, cells_z = 4, 16, 128
wide_x, wide_y = cells_x + 2, cells_y + 2
own_y = wide_y - 4
late_rows = 4 * wide_x
early_rows = wide_x * own_y
early_padded = 88
tile_rows = 112
x_rows, x_flow, y_rows, y_flow = 88, 40, 40, 16


def on_side(axis, side):
    return lax.rem(lax.axis_index(axis), 2) == side


def split_cells(cells):
    lane = cells & (cells_z - 1)
    column = cells >> 7
    i = (column * 3641) >> 16
    j = column - i * wide_y
    late = jnp.where(j < 2, j, j - own_y) * wide_x + i
    early = late_rows + i * own_y + (j - 2)
    row = jnp.where((j < 2) | (j >= wide_y - 2), late, early)
    return row, lane


def points_in(cells_ref, block):
    return jnp.concatenate([cells_ref[s, block : block + 1] for s in range(cells_ref.shape[0])], axis=0)


def halves(value):
    high = value.astype(jnp.bfloat16)
    low = (value - high.astype(jnp.float32)).astype(jnp.bfloat16)
    return high, low


def counted(rows):
    return lax.broadcasted_iota(jnp.int32, (rows, 128), 0)


def narrow(value):
    return value.astype(jnp.float32).astype(jnp.bfloat16)


def pairs_of(block, points):
    every = [(block, s) for s in range(points)]
    return [every[at : at + 2] for at in range(0, points, 2)]


def deposit_kernel(live_ref, cells_ref, volume_ref, velocity_ref, particle_ref, *refs):
    tile_ref, odd_ref, even_ref, share_ref, particle_out, cells_in, volume_in, live_in, sems = refs
    points, blocks = cells_ref.shape[0], cells_ref.shape[1]
    is_even = on_side("gx", 0)
    odd_layer = jnp.where(is_even, 0, cells_x - 1)
    even_layer = cells_x - 1 - odd_layer
    copies = [
        pltpu.make_async_copy(cells_ref, cells_in, sems.at[0]),
        pltpu.make_async_copy(volume_ref, volume_in, sems.at[1]),
        pltpu.make_async_copy(live_ref, live_in, sems.at[2]),
        pltpu.make_async_copy(particle_ref, particle_out, sems.at[9]),
    ]
    for f in range(3):
        at = pl.ds(x_flow + cells_y * f, cells_y)
        copies.append(pltpu.make_async_copy(velocity_ref.at[f, odd_layer], odd_ref.at[at], sems.at[3 + f]))
        copies.append(pltpu.make_async_copy(velocity_ref.at[f, even_layer], even_ref.at[at], sems.at[6 + f]))
    for copy in copies:
        copy.start()
    row_at = narrow(counted(tile_rows))
    lane_at = narrow(counted(cells_z))
    one = jnp.ones((), jnp.bfloat16)
    zero = jnp.zeros((), jnp.bfloat16)
    copies[1].wait()
    share = volume_in[...] / points
    high, low = halves(share)
    copies[0].wait()
    totals = []
    for b in range(blocks):
        row, lane = split_cells(points_in(cells_in, b))
        row, lane = narrow(row), narrow(lane)
        total = jnp.zeros((2 * tile_rows, cells_z), jnp.float32)
        for pair in pairs_of(b, points):
            left, right = [], []
            for _, s in pair:
                at_row = row_at == row[s : s + 1]
                left.append(
                    jnp.concatenate(
                        [jnp.where(at_row, high[b : b + 1], zero), jnp.where(at_row, low[b : b + 1], zero)], axis=0
                    )
                )
                right.append(jnp.where(lane_at == lane[s : s + 1], one, zero))
            total += lax.dot_general(
                jnp.concatenate(left, axis=1),
                jnp.concatenate(right, axis=1),
                (((1,), (1,)), ((), ())),
                preferred_element_type=jnp.float32,
            )
        totals.append(total)
    copies[2].wait()
    live = live_in[0, 0]
    tile = jnp.zeros((tile_rows, cells_z), jnp.float32)
    for b in range(blocks):
        alive = jnp.where(b < live, 1.0, 0.0)
        tile += alive * (totals[b][:tile_rows] + totals[b][tile_rows:])
        share_ref[b : b + 1] = alive * share[b : b + 1]
    tile_ref[...] = tile
    lower, upper = tile_ref[24:52], tile_ref[80:108]
    odd_ref[0:28] = jnp.where(is_even, lower, upper)
    even_ref[0:28] = jnp.where(is_even, upper, lower)
    for g in range(4):
        lower, upper = tile_ref[6 * g : 6 * g + 2], tile_ref[6 * g + 4 : 6 * g + 6]
        odd_ref[28 + 2 * g : 30 + 2 * g] = jnp.where(is_even, lower, upper)
        even_ref[28 + 2 * g : 30 + 2 * g] = jnp.where(is_even, upper, lower)
    odd_ref[36:40] = jnp.zeros((4, 128), jnp.float32)
    even_ref[36:40] = jnp.zeros((4, 128), jnp.float32)
    for copy in copies[3:]:
        copy.wait()


def middle_kernel(tile_ref, velocity_ref, odd_ref, even_ref, out_ref, up_ref, down_ref, flow_ref):
    is_even = on_side("gx", 0)

    def from_below(first, last):
        return jnp.where(is_even, odd_ref[first:last], even_ref[first:last])

    def from_above(first, last):
        return jnp.where(is_even, even_ref[first:last], odd_ref[first:last])

    out_ref[...] = tile_ref[...]
    out_ref[24:52] += from_below(0, 28)
    out_ref[80:108] += from_above(0, 28)
    for g in range(4):
        out_ref[6 * g : 6 * g + 2] += from_below(28 + 2 * g, 30 + 2 * g)
        out_ref[6 * g + 4 : 6 * g + 6] += from_above(28 + 2 * g, 30 + 2 * g)
    flow_ref[0:48] = from_below(x_flow, x_rows)
    flow_ref[48:96] = from_above(x_flow, x_rows)

    def fill(dest_ref, first, near):
        dest_ref[...] = jnp.zeros((y_rows, 128), jnp.float32)
        dest_ref[0:12] = out_ref[first : first + 12]
        for f in range(3):
            at, halo = y_flow + 8 * f, cells_y * f + near
            dest_ref[at : at + 1] = flow_ref[halo : halo + 1]
            for i in range(cells_x):
                dest_ref[at + 1 + i : at + 2 + i] = velocity_ref[f, i, near : near + 1]
            dest_ref[at + 5 : at + 6] = flow_ref[48 + halo : 49 + halo]

    fill(up_ref, 12, cells_y - 1)
    fill(down_ref, 0, 0)


def looked_up(cells_ref, fields, first):
    points, blocks = cells_ref.shape[0], cells_ref.shape[1]
    rows = fields[0].shape[0]
    table = jnp.concatenate(list(halves(jnp.concatenate(fields, axis=0))), axis=1)
    row_at = counted(rows) + first
    lane_at = narrow(counted(cells_z))
    one = jnp.ones((), jnp.bfloat16)
    zero = jnp.zeros((), jnp.bfloat16)
    sums = []
    for b in range(blocks):
        row, lane = split_cells(points_in(cells_ref, b))
        lane = narrow(lane)
        part_sums = [jnp.zeros((8, 128), jnp.float32) for _ in fields]
        for pair in pairs_of(b, points):
            right = [jnp.where(lane_at == lane[s : s + 1], one, zero) for _, s in pair]
            right = jnp.concatenate(right, axis=1)
            found = jnp.dot(table, jnp.concatenate([right, right], axis=0), preferred_element_type=jnp.float32)
            for n, (_, s) in enumerate(pair):
                at_row = row_at == row[s : s + 1]
                for f in range(len(fields)):
                    part = jnp.where(at_row, found[f * rows : (f + 1) * rows, n * 128 : n * 128 + 128], 0.0)
                    part_sums[f] = part_sums[f] + jnp.sum(part.reshape(rows // 8, 8, 128), axis=0)
        sums.append([jnp.sum(part, axis=0, keepdims=True) for part in part_sums])
    return sums


def void_of(solid):
    return jnp.maximum(1.0 - solid, void_floor)


def resistance_of(void):
    return jnp.exp(exponent * jnp.log(void))


def early_kernel(side, cells_ref, velocity_ref, tile_ref, flow_ref, sums_ref):
    @pl.when(on_side("gy", side))
    def _():
        resistance = resistance_of(void_of(tile_ref[late_rows : late_rows + early_rows]))
        fields = [resistance]
        for f in range(3):
            halo = cells_y * f + 1
            flow = [flow_ref[halo : halo + own_y]]
            flow += [velocity_ref[f, i, 1 : 1 + own_y] for i in range(cells_x)]
            flow += [flow_ref[48 + halo : 48 + halo + own_y]]
            fields.append(resistance * jnp.concatenate(flow, axis=0))
        blank = jnp.zeros((early_padded - early_rows, 128), jnp.float32)
        fields = [jnp.concatenate([field, blank], axis=0) for field in fields]
        for b, sums in enumerate(looked_up(cells_ref, fields, late_rows)):
            for f in range(4):
                sums_ref[f, b : b + 1] = sums[f]


def drag_kernel(side, *refs):
    cells_ref, share_ref, particle_ref, tile_ref, up_ref, down_ref, below_ref, above_ref, sums_ref = refs[:9]
    void_out, drag_out, void_ref, drag_ref, sems = refs[-5:]

    @pl.when(on_side("gy", side))
    def _():
        late = jnp.concatenate([tile_ref[0:12] + below_ref[0:12], tile_ref[12:24] + above_ref[0:12]], axis=0)
        late_void = void_of(late)
        early_void = void_of(tile_ref[late_rows : late_rows + early_rows])
        for i in range(1, cells_x + 1):
            void_ref[i - 1, 0:1] = late_void[wide_x + i : wide_x + i + 1]
            void_ref[i - 1, 1 : 1 + own_y] = early_void[i * own_y : (i + 1) * own_y]
            void_ref[i - 1, 1 + own_y : 2 + own_y] = late_void[2 * wide_x + i : 2 * wide_x + i + 1]
        resistance = resistance_of(late_void)
        fields = [resistance]
        for f in range(3):
            at = slice(y_flow + 8 * f, y_flow + 8 * f + wide_x)
            flow = jnp.concatenate([below_ref[at], down_ref[at], up_ref[at], above_ref[at]], axis=0)
            fields.append(resistance * flow)
        for b, sums in enumerate(looked_up(cells_ref, fields, 0)):
            total = [sums[f] + sums_ref[f, b : b + 1] for f in range(4)]
            for f in range(3):
                force = total[f + 1] - particle_ref[f, b : b + 1] * total[0]
                drag_ref[f, b : b + 1] = drag_scale * share_ref[b : b + 1] * force
        copies = [
            pltpu.make_async_copy(void_ref, void_out, sems.at[0]),
            pltpu.make_async_copy(drag_ref, drag_out, sems.at[1]),
        ]
        for copy in copies:
            copy.start()
        for copy in copies:
            copy.wait()


def on_chip(count):
    return [pl.BlockSpec(memory_space=pltpu.VMEM)] * count


def array_of(*shape):
    return jax.ShapeDtypeStruct(shape, jnp.float32)


def swapped(value, axis, odd):
    count = lax.axis_size(axis)
    return lax.ppermute(value, axis, [(i, (i + 1 if i % 2 == odd else i - 1) % count) for i in range(count)])


def one_way(value, axis, side, step):
    count = lax.axis_size(axis)
    return lax.ppermute(value, axis, [(i, (i + step) % count) for i in range(count) if i % 2 == side])


def early(side, values):
    return pl.pallas_call(
        functools.partial(early_kernel, side),
        out_shape=array_of(4, values[0].shape[1], 128),
        in_specs=on_chip(4),
        out_specs=on_chip(1)[0],
        compiler_params=small(),
        cost_estimate=pl.CostEstimate(flops=3_000_000_000, bytes_accessed=300_000, transcendentals=20_000),
    )(*values)


def drag_of(side, values, result):
    blocks = values[1].shape[0]
    in_hbm = pl.BlockSpec(memory_space=pltpu.HBM)
    return pl.pallas_call(
        functools.partial(drag_kernel, side),
        out_shape=(array_of(cells_x, cells_y, cells_z), array_of(3, blocks, 128)),
        in_specs=on_chip(9) + [in_hbm] * len(result),
        out_specs=(in_hbm,) * 2,
        scratch_shapes=[
            pltpu.VMEM((cells_x, cells_y, cells_z), jnp.float32),
            pltpu.VMEM((3, blocks, 128), jnp.float32),
            pltpu.SemaphoreType.DMA((2,)),
        ],
        input_output_aliases={9: 0, 10: 1} if result else {},
        compiler_params=small(),
    )(*values, *result)


def small():
    return pltpu.CompilerParams(vmem_limit_bytes=16 * 1024 * 1024)


def body(fluid_velocity, particle_velocity, particle_volume, satellite_cells, live_blocks):
    cells = jnp.transpose(satellite_cells[0, 0], (1, 0, 2))
    volume = particle_volume[0, 0]
    particles = jnp.transpose(particle_velocity[0, 0], (1, 0, 2))
    blocks = volume.shape[0]
    tile, x_odd, x_even, share, particles = pl.pallas_call(
        deposit_kernel,
        out_shape=(array_of(tile_rows, 128), array_of(x_rows, 128), array_of(x_rows, 128), array_of(blocks, 128), array_of(3, blocks, 128)),
        in_specs=[pl.BlockSpec(memory_space=pltpu.HBM)] * 5,
        out_specs=tuple(on_chip(5)),
        scratch_shapes=[
            pltpu.VMEM(cells.shape, jnp.int32),
            pltpu.VMEM(volume.shape, jnp.float32),
            pltpu.SMEM(live_blocks.shape, jnp.int32),
            pltpu.SemaphoreType.DMA((10,)),
        ],
        compiler_params=small(),
        name="deposit",
    )(live_blocks, *(pltpu.with_memory_space_constraint(value, pltpu.HBM) for value in (cells, volume, fluid_velocity, particles)))
    x_odd = swapped(x_odd, "gx", 1)
    x_even = swapped(x_even, "gx", 0)
    tile, y_up, y_down, flow = pl.pallas_call(
        middle_kernel,
        out_shape=(array_of(tile_rows, 128), array_of(y_rows, 128), array_of(y_rows, 128), array_of(96, 128)),
        in_specs=on_chip(4),
        out_specs=tuple(on_chip(4)),
        compiler_params=small(),
        name="middle",
    )(tile, fluid_velocity, x_odd, x_even)
    below_even = one_way(y_up, "gy", 1, 1)
    above_even = one_way(y_down, "gy", 1, -1)
    early_in = (cells, fluid_velocity, tile, flow)
    sums_even = early(0, early_in)
    below_odd = one_way(y_up, "gy", 0, 1)
    above_odd = one_way(y_down, "gy", 0, -1)
    sums_odd = early(1, early_in)
    rest = (cells, share, particles, tile, y_up, y_down)
    result = drag_of(0, rest + (below_even, above_even, sums_even), ())
    void, drag = drag_of(1, rest + (below_odd, above_odd, sums_odd), result)
    return void, jnp.transpose(drag, (1, 0, 2))[None, None]


def solution(mesh):
    placed = (
        P(None, "gx", "gy", None),
        P("gx", "gy", None, None, None),
        P("gx", "gy", None, None),
        P("gx", "gy", None, None, None),
        P("gx", "gy"),
    )
    return jax.shard_map(
        body,
        mesh=mesh,
        in_specs=placed,
        out_specs=(P("gx", "gy", None), P("gx", "gy", None, None, None)),
        check_vma=False,
    )
```

```python
import functools

import jax
import jax.numpy as jnp
from jax import lax
from jax.experimental import pallas as pl
from jax.experimental.pallas import tpu as pltpu
from jax.sharding import PartitionSpec as P


exponent = -2.65
drag_scale = 2.0
void_floor = 0.1

cells_x, cells_y, cells_z = 4, 16, 128
wide_x, wide_y = cells_x + 2, cells_y + 2
own_y = wide_y - 4
late_rows = 4 * wide_x
early_rows = wide_x * own_y
early_padded = 88
tile_rows = 112
x_rows, x_flow, y_rows, y_flow = 88, 40, 40, 16


def on_side(axis, side):
    return lax.rem(lax.axis_index(axis), 2) == side


def columns_of(cells):
    lane = cells & (cells_z - 1)
    column = cells >> 7
    i = (column * 3641) >> 16
    return i, column - i * wide_y, lane


def split_cells(cells):
    i, j, lane = columns_of(cells)
    late = jnp.where(j < 2, j, j - own_y) * wide_x + i
    early = late_rows + i * own_y + (j - 2)
    row = jnp.where((j < 2) | (j >= wide_y - 2), late, early)
    return row, lane


def points_in(cells_ref, block):
    return jnp.concatenate([cells_ref[s, block : block + 1] for s in range(cells_ref.shape[0])], axis=0)


def halves(value):
    high = value.astype(jnp.bfloat16)
    low = (value - high.astype(jnp.float32)).astype(jnp.bfloat16)
    return high, low


def counted(rows):
    return lax.broadcasted_iota(jnp.int32, (rows, 128), 0)


def narrow(value):
    return value.astype(jnp.float32).astype(jnp.bfloat16)


def pairs_of(block, points):
    every = [(block, s) for s in range(points)]
    return [every[at : at + 2] for at in range(0, points, 2)]


def deposited(cells_ref, high, low, row_of, rows):
    points, blocks = cells_ref.shape[0], cells_ref.shape[1]
    row_at = narrow(counted(rows))
    lane_at = narrow(counted(cells_z))
    one = jnp.ones((), jnp.bfloat16)
    zero = jnp.zeros((), jnp.bfloat16)
    total = jnp.zeros((2 * rows, cells_z), jnp.float32)
    for b in range(blocks):
        i, j, lane = columns_of(points_in(cells_ref, b))
        row, lane = narrow(row_of(i, j)), narrow(lane)
        for pair in pairs_of(b, points):
            left, right = [], []
            for _, s in pair:
                at_row = row_at == row[s : s + 1]
                left.append(
                    jnp.concatenate(
                        [jnp.where(at_row, high[b : b + 1], zero), jnp.where(at_row, low[b : b + 1], zero)], axis=0
                    )
                )
                right.append(jnp.where(lane_at == lane[s : s + 1], one, zero))
            total += lax.dot_general(
                jnp.concatenate(left, axis=1),
                jnp.concatenate(right, axis=1),
                (((1,), (1,)), ((), ())),
                preferred_element_type=jnp.float32,
            )
    return total[:rows] + total[rows:]


def layer_row(i, j):
    early = i * own_y + j - 2
    late = 2 * own_y + jnp.where(j < 2, j, j - own_y) * 2 + i
    return jnp.where(is_late(j), late, early)


def is_late(j):
    return (j < 2) | (j >= wide_y - 2)


def outer_row(i, j):
    upper = i >= cells_x
    row = layer_row(jnp.where(upper, i - cells_x, i), j) + jnp.where(upper, 36, 0)
    inner = jnp.where(is_late(j), layer_row(i - 2, j) + 44, 127)
    return jnp.where((i == 2) | (i == 3), inner, row)


def inner_row(i, j):
    return jnp.where(((i == 2) | (i == 3)) & ~is_late(j), layer_row(i - 2, j), 127)


def deposit_kernel(live_ref, cells_ref, volume_ref, velocity_ref, particle_ref, *refs):
    odd_ref, even_ref, late_ref, share_ref, particle_out, cells_in, volume_in, sems = refs
    points, blocks = cells_ref.shape[0], cells_ref.shape[1]
    is_even = on_side("gx", 0)
    odd_layer = jnp.where(is_even, 0, cells_x - 1)
    even_layer = cells_x - 1 - odd_layer
    copies = [
        pltpu.make_async_copy(cells_ref, cells_in, sems.at[0]),
        pltpu.make_async_copy(volume_ref, volume_in, sems.at[1]),
        pltpu.make_async_copy(particle_ref, particle_out, sems.at[2]),
    ]
    for f in range(3):
        at = pl.ds(x_flow + cells_y * f, cells_y)
        copies.append(pltpu.make_async_copy(velocity_ref.at[f, odd_layer], odd_ref.at[at], sems.at[3 + f]))
        copies.append(pltpu.make_async_copy(velocity_ref.at[f, even_layer], even_ref.at[at], sems.at[6 + f]))
    for copy in copies:
        copy.start()
    live = live_ref[0, 0]
    copies[1].wait()
    for b in range(blocks):
        share_ref[b : b + 1] = jnp.where(b < live, 1.0, 0.0) * volume_in[b : b + 1] / points
    copies[0].wait()
    high, low = halves(share_ref[...])
    total = deposited(cells_in, high, low, outer_row, 80)
    late_ref[...] = total[72:80]
    lower, upper = total[0:36], total[36:72]
    odd_ref[0:36] = jnp.where(is_even, lower, upper)
    even_ref[0:36] = jnp.where(is_even, upper, lower)
    odd_ref[36:40] = jnp.zeros((4, 128), jnp.float32)
    even_ref[36:40] = jnp.zeros((4, 128), jnp.float32)
    for copy in copies[2:]:
        copy.wait()


def middle_kernel(late_ref, velocity_ref, *refs):
    sent_odd_ref, sent_even_ref, odd_ref, even_ref, out_ref, up_ref, down_ref, flow_ref = refs
    is_even = on_side("gx", 0)

    def from_below(first, last):
        return jnp.where(is_even, odd_ref[first:last], even_ref[first:last])

    def from_above(first, last):
        return jnp.where(is_even, even_ref[first:last], odd_ref[first:last])

    def all_lower(first, last):
        return jnp.where(is_even, sent_odd_ref[first:last], sent_even_ref[first:last]) + from_below(first, last)

    def all_upper(first, last):
        return jnp.where(is_even, sent_even_ref[first:last], sent_odd_ref[first:last]) + from_above(first, last)

    out_ref[24:52] = all_lower(0, 28)
    out_ref[52:80] = jnp.zeros((28, 128), jnp.float32)
    out_ref[80:108] = all_upper(0, 28)
    out_ref[108:112] = jnp.zeros((4, 128), jnp.float32)
    for g in range(4):
        at = slice(28 + 2 * g, 30 + 2 * g)
        out_ref[6 * g : 6 * g + 2] = all_lower(at.start, at.stop)
        out_ref[6 * g + 2 : 6 * g + 4] = late_ref[2 * g : 2 * g + 2]
        out_ref[6 * g + 4 : 6 * g + 6] = all_upper(at.start, at.stop)
    flow_ref[0:48] = from_below(x_flow, x_rows)
    flow_ref[48:96] = from_above(x_flow, x_rows)

    def fill(dest_ref, first, near):
        dest_ref[...] = jnp.zeros((y_rows, 128), jnp.float32)
        dest_ref[0:12] = out_ref[first : first + 12]
        for f in range(3):
            at, halo = y_flow + 8 * f, cells_y * f + near
            dest_ref[at : at + 1] = flow_ref[halo : halo + 1]
            for i in range(cells_x):
                dest_ref[at + 1 + i : at + 2 + i] = velocity_ref[f, i, near : near + 1]
            dest_ref[at + 5 : at + 6] = flow_ref[48 + halo : 49 + halo]

    fill(up_ref, 12, cells_y - 1)
    fill(down_ref, 0, 0)


def looked_up(cells_ref, fields, first):
    points, blocks = cells_ref.shape[0], cells_ref.shape[1]
    rows = fields[0].shape[0]
    table = jnp.concatenate(list(halves(jnp.concatenate(fields, axis=0))), axis=1)
    row_at = counted(rows) + first
    lane_at = narrow(counted(cells_z))
    one = jnp.ones((), jnp.bfloat16)
    zero = jnp.zeros((), jnp.bfloat16)
    sums = []
    for b in range(blocks):
        row, lane = split_cells(points_in(cells_ref, b))
        lane = narrow(lane)
        part_sums = [jnp.zeros((8, 128), jnp.float32) for _ in fields]
        for pair in pairs_of(b, points):
            right = [jnp.where(lane_at == lane[s : s + 1], one, zero) for _, s in pair]
            right = jnp.concatenate(right, axis=1)
            found = jnp.dot(table, jnp.concatenate([right, right], axis=0), preferred_element_type=jnp.float32)
            for n, (_, s) in enumerate(pair):
                at_row = row_at == row[s : s + 1]
                for f in range(len(fields)):
                    part = jnp.where(at_row, found[f * rows : (f + 1) * rows, n * 128 : n * 128 + 128], 0.0)
                    part_sums[f] = part_sums[f] + jnp.sum(part.reshape(rows // 8, 8, 128), axis=0)
        sums.append([jnp.sum(part, axis=0, keepdims=True) for part in part_sums])
    return sums


def void_of(solid):
    return jnp.maximum(1.0 - solid, void_floor)


def resistance_of(void):
    return jnp.exp(exponent * jnp.log(void))


def early_void_of(tile_ref, inner_ref):
    return void_of(jnp.concatenate([tile_ref[24:52], inner_ref[0:28], tile_ref[80:108]], axis=0))


def early_kernel(side, cells_ref, share_ref, velocity_ref, tile_ref, flow_ref, sums_ref, inner_ref):
    @pl.when(on_side("gy", side))
    def _():
        high, low = halves(share_ref[...])
        inner_ref[...] = deposited(cells_ref, high, low, inner_row, 32)
        resistance = resistance_of(early_void_of(tile_ref, inner_ref))
        fields = [resistance]
        for f in range(3):
            halo = cells_y * f + 1
            flow = [flow_ref[halo : halo + own_y]]
            flow += [velocity_ref[f, i, 1 : 1 + own_y] for i in range(cells_x)]
            flow += [flow_ref[48 + halo : 48 + halo + own_y]]
            fields.append(resistance * jnp.concatenate(flow, axis=0))
        blank = jnp.zeros((early_padded - early_rows, 128), jnp.float32)
        fields = [jnp.concatenate([field, blank], axis=0) for field in fields]
        for b, sums in enumerate(looked_up(cells_ref, fields, late_rows)):
            for f in range(4):
                sums_ref[f, b : b + 1] = sums[f]


def drag_kernel(side, *refs):
    cells_ref, share_ref, particle_ref, tile_ref, up_ref, down_ref, below_ref, above_ref, sums_ref, inner_ref = refs[:10]
    void_out, drag_out, void_ref, drag_ref, sems = refs[-5:]

    @pl.when(on_side("gy", side))
    def _():
        late = jnp.concatenate([tile_ref[0:12] + below_ref[0:12], tile_ref[12:24] + above_ref[0:12]], axis=0)
        late_void = void_of(late)
        early_void = early_void_of(tile_ref, inner_ref)
        for i in range(1, cells_x + 1):
            void_ref[i - 1, 0:1] = late_void[wide_x + i : wide_x + i + 1]
            void_ref[i - 1, 1 : 1 + own_y] = early_void[i * own_y : (i + 1) * own_y]
            void_ref[i - 1, 1 + own_y : 2 + own_y] = late_void[2 * wide_x + i : 2 * wide_x + i + 1]
        resistance = resistance_of(late_void)
        fields = [resistance]
        for f in range(3):
            at = slice(y_flow + 8 * f, y_flow + 8 * f + wide_x)
            flow = jnp.concatenate([below_ref[at], down_ref[at], up_ref[at], above_ref[at]], axis=0)
            fields.append(resistance * flow)
        for b, sums in enumerate(looked_up(cells_ref, fields, 0)):
            total = [sums[f] + sums_ref[f, b : b + 1] for f in range(4)]
            for f in range(3):
                force = total[f + 1] - particle_ref[f, b : b + 1] * total[0]
                drag_ref[f, b : b + 1] = drag_scale * share_ref[b : b + 1] * force
        copies = [
            pltpu.make_async_copy(void_ref, void_out, sems.at[0]),
            pltpu.make_async_copy(drag_ref, drag_out, sems.at[1]),
        ]
        for copy in copies:
            copy.start()
        for copy in copies:
            copy.wait()


def on_chip(count):
    return [pl.BlockSpec(memory_space=pltpu.VMEM)] * count


def array_of(*shape):
    return jax.ShapeDtypeStruct(shape, jnp.float32)


def swapped(value, axis, odd):
    count = lax.axis_size(axis)
    return lax.ppermute(value, axis, [(i, (i + 1 if i % 2 == odd else i - 1) % count) for i in range(count)])


def one_way(value, axis, side, step):
    count = lax.axis_size(axis)
    return lax.ppermute(value, axis, [(i, (i + step) % count) for i in range(count) if i % 2 == side])


def early(side, values):
    return pl.pallas_call(
        functools.partial(early_kernel, side),
        out_shape=(array_of(4, values[0].shape[1], 128), array_of(32, 128)),
        in_specs=on_chip(5),
        out_specs=tuple(on_chip(2)),
        compiler_params=small(),
        cost_estimate=pl.CostEstimate(flops=3_000_000_000, bytes_accessed=300_000, transcendentals=20_000),
    )(*values)


def drag_of(side, values, result):
    blocks = values[1].shape[0]
    in_hbm = pl.BlockSpec(memory_space=pltpu.HBM)
    return pl.pallas_call(
        functools.partial(drag_kernel, side),
        out_shape=(array_of(cells_x, cells_y, cells_z), array_of(3, blocks, 128)),
        in_specs=on_chip(10) + [in_hbm] * len(result),
        out_specs=(in_hbm,) * 2,
        scratch_shapes=[
            pltpu.VMEM((cells_x, cells_y, cells_z), jnp.float32),
            pltpu.VMEM((3, blocks, 128), jnp.float32),
            pltpu.SemaphoreType.DMA((2,)),
        ],
        input_output_aliases={10: 0, 11: 1} if result else {},
        compiler_params=small(),
    )(*values, *result)


def small():
    return pltpu.CompilerParams(vmem_limit_bytes=16 * 1024 * 1024)


def body(fluid_velocity, particle_velocity, particle_volume, satellite_cells, live_blocks):
    cells = jnp.transpose(satellite_cells[0, 0], (1, 0, 2))
    volume = particle_volume[0, 0]
    particles = jnp.transpose(particle_velocity[0, 0], (1, 0, 2))
    blocks = volume.shape[0]
    fetched = (pltpu.with_memory_space_constraint(value, pltpu.HBM) for value in (cells, volume, fluid_velocity, particles))
    x_odd, x_even, late, share, particles = pl.pallas_call(
        deposit_kernel,
        out_shape=tuple(array_of(rows, 128) for rows in (x_rows, x_rows, 8, blocks)) + (array_of(3, blocks, 128),),
        in_specs=[pl.BlockSpec(memory_space=pltpu.SMEM)] + [pl.BlockSpec(memory_space=pltpu.HBM)] * 4,
        out_specs=tuple(on_chip(5)),
        scratch_shapes=[
            pltpu.VMEM(cells.shape, jnp.int32),
            pltpu.VMEM(volume.shape, jnp.float32),
            pltpu.SemaphoreType.DMA((9,)),
        ],
        compiler_params=small(),
        name="deposit",
    )(live_blocks, *fetched)
    from_odd = swapped(x_odd, "gx", 1)
    from_even = swapped(x_even, "gx", 0)
    tile, y_up, y_down, flow = pl.pallas_call(
        middle_kernel,
        out_shape=(array_of(tile_rows, 128), array_of(y_rows, 128), array_of(y_rows, 128), array_of(96, 128)),
        in_specs=on_chip(6),
        out_specs=tuple(on_chip(4)),
        compiler_params=small(),
        name="middle",
    )(late, fluid_velocity, x_odd, x_even, from_odd, from_even)
    below_even = one_way(y_up, "gy", 1, 1)
    above_even = one_way(y_down, "gy", 1, -1)
    early_in = (cells, share, fluid_velocity, tile, flow)
    sums_even = early(0, early_in)
    below_odd = one_way(y_up, "gy", 0, 1)
    above_odd = one_way(y_down, "gy", 0, -1)
    sums_odd = early(1, early_in)
    rest = (cells, share, particles, tile, y_up, y_down)
    result = drag_of(0, rest + (below_even, above_even, *sums_even), ())
    void, drag = drag_of(1, rest + (below_odd, above_odd, *sums_odd), result)
    return void, jnp.transpose(drag, (1, 0, 2))[None, None]


def solution(mesh):
    placed = (
        P(None, "gx", "gy", None),
        P("gx", "gy", None, None, None),
        P("gx", "gy", None, None),
        P("gx", "gy", None, None, None),
        P("gx", "gy"),
    )
    return jax.shard_map(
        body,
        mesh=mesh,
        in_specs=placed,
        out_specs=(P("gx", "gy", None), P("gx", "gy", None, None, None)),
        check_vma=False,
    )
```

```python
import functools

import jax
import jax.numpy as jnp
from jax import lax
from jax.experimental import pallas as pl
from jax.experimental.pallas import tpu as pltpu
from jax.sharding import PartitionSpec as P


exponent = -2.65
drag_scale = 2.0
void_floor = 0.1

cells_x, cells_y, cells_z = 4, 16, 128
wide_x, wide_y = cells_x + 2, cells_y + 2
own_y = wide_y - 4
late_rows = 4 * wide_x
early_rows = wide_x * own_y
early_padded = 88
tile_rows = 112
x_rows, x_flow, y_rows, y_flow = 88, 40, 40, 16


def on_side(axis, side):
    return lax.rem(lax.axis_index(axis), 2) == side


def columns_of(cells):
    lane = cells & (cells_z - 1)
    column = cells >> 7
    i = (column * 3641) >> 16
    return i, column - i * wide_y, lane


def split_cells(cells):
    i, j, lane = columns_of(cells)
    late = jnp.where(j < 2, j, j - own_y) * wide_x + i
    early = late_rows + i * own_y + (j - 2)
    row = jnp.where((j < 2) | (j >= wide_y - 2), late, early)
    return row, lane


def points_in(cells_ref, block):
    return jnp.concatenate([cells_ref[s, block : block + 1] for s in range(cells_ref.shape[0])], axis=0)


def halves(value):
    high = value.astype(jnp.bfloat16)
    low = (value - high.astype(jnp.float32)).astype(jnp.bfloat16)
    return high, low


def counted(rows):
    return lax.broadcasted_iota(jnp.int32, (rows, 128), 0)


def narrow(value):
    return value.astype(jnp.float32).astype(jnp.bfloat16)


def pairs_of(block, points):
    every = [(block, s) for s in range(points)]
    return [every[at : at + 2] for at in range(0, points, 2)]


def deposited(cells_ref, high, low, row_of, rows):
    points, blocks = cells_ref.shape[0], cells_ref.shape[1]
    row_at = narrow(counted(rows))
    lane_at = narrow(counted(cells_z))
    one = jnp.ones((), jnp.bfloat16)
    zero = jnp.zeros((), jnp.bfloat16)
    total = jnp.zeros((2 * rows, cells_z), jnp.float32)
    for b in range(blocks):
        i, j, lane = columns_of(points_in(cells_ref, b))
        row, lane = narrow(row_of(i, j)), narrow(lane)
        for pair in pairs_of(b, points):
            left, right = [], []
            for _, s in pair:
                at_row = row_at == row[s : s + 1]
                left.append(
                    jnp.concatenate(
                        [jnp.where(at_row, high[b : b + 1], zero), jnp.where(at_row, low[b : b + 1], zero)], axis=0
                    )
                )
                right.append(jnp.where(lane_at == lane[s : s + 1], one, zero))
            total += lax.dot_general(
                jnp.concatenate(left, axis=1),
                jnp.concatenate(right, axis=1),
                (((1,), (1,)), ((), ())),
                preferred_element_type=jnp.float32,
            )
    return total[:rows] + total[rows:]


def layer_row(i, j):
    early = i * own_y + j - 2
    late = 2 * own_y + jnp.where(j < 2, j, j - own_y) * 2 + i
    return jnp.where(is_late(j), late, early)


def is_late(j):
    return (j < 2) | (j >= wide_y - 2)


def outer_row(i, j):
    upper = i >= cells_x
    row = layer_row(jnp.where(upper, i - cells_x, i), j) + jnp.where(upper, 36, 0)
    inner = jnp.where(is_late(j), layer_row(i - 2, j) + 44, 127)
    return jnp.where((i == 2) | (i == 3), inner, row)


def inner_row(i, j):
    return jnp.where(((i == 2) | (i == 3)) & ~is_late(j), layer_row(i - 2, j), 127)


def deposit_kernel(live_ref, cells_ref, volume_ref, velocity_ref, particle_ref, *refs):
    odd_ref, even_ref, late_ref, share_ref, particle_out, cells_in, volume_in, sems = refs
    points, blocks = cells_ref.shape[0], cells_ref.shape[1]
    is_even = on_side("gx", 0)
    odd_layer = jnp.where(is_even, 0, cells_x - 1)
    even_layer = cells_x - 1 - odd_layer
    copies = [
        pltpu.make_async_copy(cells_ref, cells_in, sems.at[0]),
        pltpu.make_async_copy(volume_ref, volume_in, sems.at[1]),
        pltpu.make_async_copy(particle_ref, particle_out, sems.at[2]),
    ]
    for f in range(3):
        at = pl.ds(x_flow + cells_y * f, cells_y)
        copies.append(pltpu.make_async_copy(velocity_ref.at[f, odd_layer], odd_ref.at[at], sems.at[3 + f]))
        copies.append(pltpu.make_async_copy(velocity_ref.at[f, even_layer], even_ref.at[at], sems.at[6 + f]))
    for copy in copies:
        copy.start()
    live = live_ref[0, 0]
    copies[1].wait()
    for b in range(blocks):
        share_ref[b : b + 1] = jnp.where(b < live, 1.0, 0.0) * volume_in[b : b + 1] / points
    copies[0].wait()
    high, low = halves(share_ref[...])
    total = deposited(cells_in, high, low, outer_row, 80)
    late_ref[...] = total[72:80]
    lower, upper = total[0:36], total[36:72]
    odd_ref[0:36] = jnp.where(is_even, lower, upper)
    even_ref[0:36] = jnp.where(is_even, upper, lower)
    odd_ref[36:40] = jnp.zeros((4, 128), jnp.float32)
    even_ref[36:40] = jnp.zeros((4, 128), jnp.float32)
    for copy in copies[2:]:
        copy.wait()


def middle_kernel(late_ref, velocity_ref, *refs):
    sent_odd_ref, sent_even_ref, odd_ref, even_ref, out_ref, up_ref, down_ref, flow_ref = refs
    is_even = on_side("gx", 0)

    def from_below(first, last):
        return jnp.where(is_even, odd_ref[first:last], even_ref[first:last])

    def from_above(first, last):
        return jnp.where(is_even, even_ref[first:last], odd_ref[first:last])

    def all_lower(first, last):
        return jnp.where(is_even, sent_odd_ref[first:last], sent_even_ref[first:last]) + from_below(first, last)

    def all_upper(first, last):
        return jnp.where(is_even, sent_even_ref[first:last], sent_odd_ref[first:last]) + from_above(first, last)

    out_ref[24:52] = all_lower(0, 28)
    out_ref[52:80] = jnp.zeros((28, 128), jnp.float32)
    out_ref[80:108] = all_upper(0, 28)
    out_ref[108:112] = jnp.zeros((4, 128), jnp.float32)
    for g in range(4):
        at = slice(28 + 2 * g, 30 + 2 * g)
        out_ref[6 * g : 6 * g + 2] = all_lower(at.start, at.stop)
        out_ref[6 * g + 2 : 6 * g + 4] = late_ref[2 * g : 2 * g + 2]
        out_ref[6 * g + 4 : 6 * g + 6] = all_upper(at.start, at.stop)
    flow_ref[0:48] = from_below(x_flow, x_rows)
    flow_ref[48:96] = from_above(x_flow, x_rows)

    def fill(dest_ref, first, near):
        dest_ref[...] = jnp.zeros((y_rows, 128), jnp.float32)
        dest_ref[0:12] = out_ref[first : first + 12]
        for f in range(3):
            at, halo = y_flow + 8 * f, cells_y * f + near
            dest_ref[at : at + 1] = flow_ref[halo : halo + 1]
            for i in range(cells_x):
                dest_ref[at + 1 + i : at + 2 + i] = velocity_ref[f, i, near : near + 1]
            dest_ref[at + 5 : at + 6] = flow_ref[48 + halo : 49 + halo]

    fill(up_ref, 12, cells_y - 1)
    fill(down_ref, 0, 0)


def looked_up(cells_ref, fields, first):
    points, blocks = cells_ref.shape[0], cells_ref.shape[1]
    rows = fields[0].shape[0]
    table = jnp.concatenate(list(halves(jnp.concatenate(fields, axis=0))), axis=1)
    row_at = counted(rows) + first
    lane_at = narrow(counted(cells_z))
    one = jnp.ones((), jnp.bfloat16)
    zero = jnp.zeros((), jnp.bfloat16)
    sums = []
    for b in range(blocks):
        row, lane = split_cells(points_in(cells_ref, b))
        lane = narrow(lane)
        part_sums = [jnp.zeros((8, 128), jnp.float32) for _ in fields]
        for pair in pairs_of(b, points):
            right = [jnp.where(lane_at == lane[s : s + 1], one, zero) for _, s in pair]
            right = jnp.concatenate(right, axis=1)
            found = jnp.dot(table, jnp.concatenate([right, right], axis=0), preferred_element_type=jnp.float32)
            for n, (_, s) in enumerate(pair):
                at_row = row_at == row[s : s + 1]
                for f in range(len(fields)):
                    part = jnp.where(at_row, found[f * rows : (f + 1) * rows, n * 128 : n * 128 + 128], 0.0)
                    part_sums[f] = part_sums[f] + jnp.sum(part.reshape(rows // 8, 8, 128), axis=0)
        sums.append([jnp.sum(part, axis=0, keepdims=True) for part in part_sums])
    return sums


def void_of(solid):
    return jnp.maximum(1.0 - solid, void_floor)


def resistance_of(void):
    return jnp.exp(exponent * jnp.log(void))


def early_void_of(tile_ref, inner_ref):
    return void_of(jnp.concatenate([tile_ref[24:52], inner_ref[0:28], tile_ref[80:108]], axis=0))


def early_kernel(side, cells_ref, share_ref, velocity_ref, tile_ref, flow_ref, sums_ref, inner_ref):
    @pl.when(on_side("gy", side))
    def _():
        high, low = halves(share_ref[...])
        inner_ref[...] = deposited(cells_ref, high, low, inner_row, 32)
        resistance = resistance_of(early_void_of(tile_ref, inner_ref))
        fields = [resistance]
        for f in range(3):
            halo = cells_y * f + 1
            flow = [flow_ref[halo : halo + own_y]]
            flow += [velocity_ref[f, i, 1 : 1 + own_y] for i in range(cells_x)]
            flow += [flow_ref[48 + halo : 48 + halo + own_y]]
            fields.append(resistance * jnp.concatenate(flow, axis=0))
        blank = jnp.zeros((early_padded - early_rows, 128), jnp.float32)
        fields = [jnp.concatenate([field, blank], axis=0) for field in fields]
        for b, sums in enumerate(looked_up(cells_ref, fields, late_rows)):
            for f in range(4):
                sums_ref[f, b : b + 1] = sums[f]


def drag_kernel(side, *refs):
    cells_ref, share_ref, particle_ref, tile_ref, up_ref, down_ref, below_ref, above_ref, sums_ref, inner_ref = refs[:10]
    void_out, drag_out, void_ref, drag_ref, sems = refs[-5:]

    @pl.when(on_side("gy", side))
    def _():
        late = jnp.concatenate([tile_ref[0:12] + below_ref[0:12], tile_ref[12:24] + above_ref[0:12]], axis=0)
        late_void = void_of(late)
        early_void = early_void_of(tile_ref, inner_ref)
        for i in range(1, cells_x + 1):
            void_ref[i - 1, 0:1] = late_void[wide_x + i : wide_x + i + 1]
            void_ref[i - 1, 1 : 1 + own_y] = early_void[i * own_y : (i + 1) * own_y]
            void_ref[i - 1, 1 + own_y : 2 + own_y] = late_void[2 * wide_x + i : 2 * wide_x + i + 1]
        void_copy = pltpu.make_async_copy(void_ref, void_out, sems.at[0])
        void_copy.start()
        resistance = resistance_of(late_void)
        fields = [resistance]
        for f in range(3):
            at = slice(y_flow + 8 * f, y_flow + 8 * f + wide_x)
            flow = jnp.concatenate([below_ref[at], down_ref[at], up_ref[at], above_ref[at]], axis=0)
            fields.append(resistance * flow)
        for b, sums in enumerate(looked_up(cells_ref, fields, 0)):
            total = [sums[f] + sums_ref[f, b : b + 1] for f in range(4)]
            for f in range(3):
                force = total[f + 1] - particle_ref[f, b : b + 1] * total[0]
                drag_ref[f, b : b + 1] = drag_scale * share_ref[b : b + 1] * force
        drag_copy = pltpu.make_async_copy(drag_ref, drag_out, sems.at[1])
        drag_copy.start()
        drag_copy.wait()
        void_copy.wait()


def on_chip(count):
    return [pl.BlockSpec(memory_space=pltpu.VMEM)] * count


def array_of(*shape):
    return jax.ShapeDtypeStruct(shape, jnp.float32)


def swapped(value, axis, odd):
    count = lax.axis_size(axis)
    return lax.ppermute(value, axis, [(i, (i + 1 if i % 2 == odd else i - 1) % count) for i in range(count)])


def one_way(value, axis, side, step):
    count = lax.axis_size(axis)
    return lax.ppermute(value, axis, [(i, (i + step) % count) for i in range(count) if i % 2 == side])


def early(side, values):
    return pl.pallas_call(
        functools.partial(early_kernel, side),
        out_shape=(array_of(4, values[0].shape[1], 128), array_of(32, 128)),
        in_specs=on_chip(5),
        out_specs=tuple(on_chip(2)),
        compiler_params=small(),
        cost_estimate=pl.CostEstimate(flops=3_000_000_000, bytes_accessed=300_000, transcendentals=20_000),
    )(*values)


def drag_of(side, values, result):
    blocks = values[1].shape[0]
    in_hbm = pl.BlockSpec(memory_space=pltpu.HBM)
    return pl.pallas_call(
        functools.partial(drag_kernel, side),
        out_shape=(array_of(cells_x, cells_y, cells_z), array_of(3, blocks, 128)),
        in_specs=on_chip(10) + [in_hbm] * len(result),
        out_specs=(in_hbm,) * 2,
        scratch_shapes=[
            pltpu.VMEM((cells_x, cells_y, cells_z), jnp.float32),
            pltpu.VMEM((3, blocks, 128), jnp.float32),
            pltpu.SemaphoreType.DMA((2,)),
        ],
        input_output_aliases={10: 0, 11: 1} if result else {},
        compiler_params=small(),
    )(*values, *result)


def small():
    return pltpu.CompilerParams(vmem_limit_bytes=16 * 1024 * 1024)


def body(fluid_velocity, particle_velocity, particle_volume, satellite_cells, live_blocks):
    cells = jnp.transpose(satellite_cells[0, 0], (1, 0, 2))
    volume = particle_volume[0, 0]
    particles = jnp.transpose(particle_velocity[0, 0], (1, 0, 2))
    blocks = volume.shape[0]
    fetched = (pltpu.with_memory_space_constraint(value, pltpu.HBM) for value in (cells, volume, fluid_velocity, particles))
    x_odd, x_even, late, share, particles = pl.pallas_call(
        deposit_kernel,
        out_shape=tuple(array_of(rows, 128) for rows in (x_rows, x_rows, 8, blocks)) + (array_of(3, blocks, 128),),
        in_specs=[pl.BlockSpec(memory_space=pltpu.SMEM)] + [pl.BlockSpec(memory_space=pltpu.HBM)] * 4,
        out_specs=tuple(on_chip(5)),
        scratch_shapes=[
            pltpu.VMEM(cells.shape, jnp.int32),
            pltpu.VMEM(volume.shape, jnp.float32),
            pltpu.SemaphoreType.DMA((9,)),
        ],
        compiler_params=small(),
        name="deposit",
    )(live_blocks, *fetched)
    from_odd = swapped(x_odd, "gx", 1)
    from_even = swapped(x_even, "gx", 0)
    tile, y_up, y_down, flow = pl.pallas_call(
        middle_kernel,
        out_shape=(array_of(tile_rows, 128), array_of(y_rows, 128), array_of(y_rows, 128), array_of(96, 128)),
        in_specs=on_chip(6),
        out_specs=tuple(on_chip(4)),
        compiler_params=small(),
        name="middle",
    )(late, fluid_velocity, x_odd, x_even, from_odd, from_even)
    below_even = one_way(y_up, "gy", 1, 1)
    above_even = one_way(y_down, "gy", 1, -1)
    early_in = (cells, share, fluid_velocity, tile, flow)
    sums_even = early(0, early_in)
    below_odd = one_way(y_up, "gy", 0, 1)
    above_odd = one_way(y_down, "gy", 0, -1)
    sums_odd = early(1, early_in)
    rest = (cells, share, particles, tile, y_up, y_down)
    result = drag_of(0, rest + (below_even, above_even, *sums_even), ())
    void, drag = drag_of(1, rest + (below_odd, above_odd, *sums_odd), result)
    return void, jnp.transpose(drag, (1, 0, 2))[None, None]


def solution(mesh):
    placed = (
        P(None, "gx", "gy", None),
        P("gx", "gy", None, None, None),
        P("gx", "gy", None, None),
        P("gx", "gy", None, None, None),
        P("gx", "gy"),
    )
    return jax.shard_map(
        body,
        mesh=mesh,
        in_specs=placed,
        out_specs=(P("gx", "gy", None), P("gx", "gy", None, None, None)),
        check_vma=False,
    )
```
